32 devices in a mesh: rows: 8 (over y, x, core), cols: 4 (over z).
Axes of the slice: x: 2, y: 2, z: 4, core: 2. Of those that a mesh axis runs over, the one named last changes fastest.
Arguments:
- intensity: float32 [4096, 4096], P('rows', 'cols'), may hold values from -0.5 to 1.5, as said below
- edge_weight: float32 [4096, 4096], P('rows', 'cols'), may hold values from 0.2 to 2
- labels: int32 [4096, 4096], P('rows', 'cols'), may hold values from 0 to 1
- tile_cost: int32 [16, 16], replicated, may hold values from 0 to 3, as said below
- tile_owner: int32 [16, 16], replicated, may hold values from -1 to 31, as said below
Outputs:
- slot_field: float32 [32, 4, 256, 256], P('rows', 'cols')
The draws below stay inside these ranges and needn't reach their ends.
Inputs may be any that keep to these rules, and one draw needn't show every extreme that they name: `intensity`: intensity of stained tissue. `tile_cost`: 0 marks a background tile, 1 to 3 a tissue tile. `tile_owner`: -1 exactly for background tiles. A tissue tile's value is k * 4 + s: it goes to slot s of the device with rows index k in its own column band; within one band no two tiles share a value; the tiles of one device's block send at most 1 tile to any one device, and in every draw some block sends exactly 1 to one device and some device receives all 4 of its slots filled.
All inputs are finite; a program needn't handle non-finite values.
Results may differ from the reference program's by a relative error of at most 0.0001.
Values sent between devices are 32-bit elements; how exact they have to be, the bound alone decides.
A program may use at most 128 MiB of HBM per device.

```python
import math
import jax
import jax.numpy as jnp

TILE = 256
BLOCK_ROWS = 512
BLOCK_COLS = 1024
ITERS_BEFORE = 2
ITERS_AFTER = 2
TILE_SLOTS = 4
ROWS = 4096
COLS = 4096
TILE_ROWS = 16
TILE_COLS = 16
N_ROWS = 8
N_COLS = 4


def tissue_plan(key):
    base_key = jax.random.fold_in(key, 4242)
    key_count, key_pick, key_start, key_level = jax.random.split(base_key, 4)
    per_row = BLOCK_COLS // TILE
    stripes = COLS // BLOCK_COLS
    devices = ROWS // BLOCK_ROWS
    stripe_total = TILE_ROWS * per_row
    half_count = stripe_total // 2
    low_count = 3 * stripe_total // 8
    counts = jax.random.randint(key_count, (stripes,), low_count, half_count + 1)
    forced = jax.random.randint(key_pick, (), 0, stripes)
    counts = jnp.where(jnp.arange(stripes) == forced, half_count, counts)
    starts = jax.random.randint(key_start, (stripes,), 0, 1 << 20) % (stripe_total - counts + 1)
    row_ids = jnp.arange(TILE_ROWS, dtype=jnp.int32)[:, None]
    col_ids = jnp.arange(TILE_COLS, dtype=jnp.int32)[None, :]
    stripe = col_ids // per_row
    run_order = row_ids * per_row + col_ids % per_row - starts[stripe]
    active = (run_order >= 0) & (run_order < counts[stripe])
    levels = jax.random.randint(key_level, (TILE_ROWS, TILE_COLS), 1, 4)
    cost_table = jnp.where(active, levels, 0).astype(jnp.int32)
    owner_table = jnp.where(active, run_order % devices * TILE_SLOTS + run_order // devices, -1).astype(jnp.int32)
    return (cost_table, owner_table)


def draw_tile_cost(key, part):
    return tissue_plan(key)[0]


def draw_tile_owner(key, part):
    return tissue_plan(key)[1]


def label_field(key):
    return (jax.random.randint(jax.random.fold_in(key, 99), (ROWS, COLS), 0, 5) < 2).astype(jnp.int32)


def draw_labels(key, part):
    return label_field(key)


def draw_intensity(key, part):
    label_cells = label_field(key).astype(jnp.float32)
    level_key = jax.random.fold_in(key, 23)
    key_gap, key_sign, key_freq, key_phase, key_amp = jax.random.split(level_key, 5)
    gaps = jax.random.uniform(key_gap, (2,), jnp.float32, 0.05, 0.15)
    signs = jnp.where(jax.random.randint(key_sign, (2,), 0, 2) == 0, -1.0, 1.0).astype(jnp.float32)
    upper_mean = 0.7 + signs[0] * gaps[0]
    lower_mean = 0.3 + signs[1] * gaps[1]
    freqs = jax.random.randint(key_freq, (3, 2), 1, 4).astype(jnp.float32)
    phases = jax.random.uniform(key_phase, (3, 2), jnp.float32, -jnp.pi, jnp.pi)
    amps = jax.random.uniform(key_amp, (3,), jnp.float32, 0.03, 0.05)
    row_pos = jnp.arange(ROWS, dtype=jnp.float32)[:, None] / ROWS
    col_pos = jnp.arange(COLS, dtype=jnp.float32)[None, :] / COLS
    smooth = jnp.zeros((ROWS, COLS), jnp.float32)
    for index in range(3):
        row_wave = jnp.cos(2.0 * jnp.pi * freqs[index, 0] * row_pos + phases[index, 0])
        col_wave = jnp.cos(2.0 * jnp.pi * freqs[index, 1] * col_pos + phases[index, 1])
        smooth = smooth + amps[index] * row_wave * col_wave
    base = lower_mean + (upper_mean - lower_mean) * label_cells + smooth
    noise_key = jax.random.fold_in(key, 17)
    noise = 0.2 * jax.random.normal(noise_key, (ROWS, COLS), jnp.float32)
    return jnp.clip(base + noise, -0.5, 1.5)


def block_scale(stream_key, dims, shards, least, largest):
    factor_of = 1.0
    for axis_at, parts in shards:
        heights = jax.random.uniform(jax.random.fold_in(jax.random.fold_in(stream_key, 6), axis_at), (parts,), jnp.float32, least / len(shards), largest / len(shards))
        factor_of = factor_of * jnp.repeat(jnp.exp(heights), dims[axis_at] // parts).reshape((-1,) + (1,) * (len(dims) - 1 - axis_at))
    return factor_of


def setup_inputs(seed: int = 0) -> dict:
    seeds = jax.random.split(jax.random.key(seed), 6)
    return {
        "intensity": draw_intensity(jax.random.fold_in(seeds[5], 71), 0),
        "edge_weight": jnp.clip(jnp.exp(math.log(2.0) - 2.3025851 * jax.random.uniform(seeds[1], (ROWS, COLS), jnp.float32) ** block_scale(seeds[1], (ROWS, COLS), ((0, 8), (1, 4)), -0.2, 0.2)), 0.2, 2.0),
        "labels": draw_labels(jax.random.fold_in(seeds[5], 71), 0),
        "tile_cost": draw_tile_cost(jax.random.fold_in(seeds[5], 71), 0),
        "tile_owner": draw_tile_owner(jax.random.fold_in(seeds[5], 71), 0),
    }


sigma_step = 0.35
tau_step = 0.35
fidelity = 1.0

def forward_diffs(field):
    grad_down = jnp.concatenate([field[1:] - field[:-1], jnp.zeros_like(field[:1])], axis=0)
    grad_right = jnp.concatenate([field[:, 1:] - field[:, :-1], jnp.zeros_like(field[:, :1])], axis=1)
    return (grad_down, grad_right)

def divergence(flux_down, flux_right):
    above_rim = jnp.concatenate([jnp.zeros_like(flux_down[:1]), flux_down[:-1]], axis=0)
    left_rim = jnp.concatenate([jnp.zeros_like(flux_right[:, :1]), flux_right[:, :-1]], axis=1)
    return flux_down - above_rim + flux_right - left_rim

def expand(table):
    return jnp.repeat(jnp.repeat(table, TILE, axis=0), TILE, axis=1)

def reference(intensity, edge_weight, labels, tile_cost, tile_owner):
    weight_cells = fidelity * expand(tile_cost.astype(jnp.float32))
    tissue = expand(tile_cost > 0)
    relaxed = labels.astype(jnp.float32)
    extrapolated = relaxed
    flux_down = jnp.zeros_like(relaxed)
    flux_right = jnp.zeros_like(relaxed)
    for iteration in range(ITERS_BEFORE + ITERS_AFTER):
        if iteration >= ITERS_BEFORE:
            frozen = jnp.logical_not(tissue)
        else:
            frozen = jnp.zeros(relaxed.shape, bool)
        inside = jnp.sum(relaxed * intensity)
        mass_in = jnp.sum(relaxed)
        outside = jnp.sum((1.0 - relaxed) * intensity)
        mass_out = jnp.sum(1.0 - relaxed)
        region = (intensity - inside / mass_in) ** 2 - (intensity - outside / mass_out) ** 2
        leading = jnp.where(frozen, relaxed, extrapolated)
        grad_down, grad_right = forward_diffs(leading)
        trial_down = flux_down + sigma_step * grad_down
        trial_right = flux_right + sigma_step * grad_right
        length = jnp.sqrt(trial_down * trial_down + trial_right * trial_right)
        shrink = jnp.maximum(1.0, length / edge_weight)
        flux_down = jnp.where(frozen, flux_down, trial_down / shrink)
        flux_right = jnp.where(frozen, flux_right, trial_right / shrink)
        updated = jnp.clip(relaxed + tau_step * (divergence(flux_down, flux_right) - weight_cells * region), 0.0, 1.0)
        updated = jnp.where(frozen, relaxed, updated)
        extrapolated = 2.0 * updated - relaxed
        relaxed = updated
    slot_count = N_ROWS * TILE_SLOTS
    tile_set = relaxed.reshape(TILE_ROWS, TILE, TILE_COLS, TILE).transpose(0, 2, 1, 3)
    stripe = (jnp.arange(TILE_COLS, dtype=jnp.int32) // (BLOCK_COLS // TILE)).astype(jnp.int32)
    stripe_ids = jnp.broadcast_to(stripe[None, :], (TILE_ROWS, TILE_COLS))
    target = jnp.where(tile_owner >= 0, tile_owner, slot_count).astype(jnp.int32)
    result = jnp.zeros((slot_count, N_COLS, TILE, TILE), jnp.float32)
    return result.at[target, stripe_ids].set(tile_set, mode='drop')
```

```python
import functools

import jax
import jax.numpy as jnp
from jax import lax
from jax.experimental import pallas as pl
from jax.experimental.pallas import tpu as pltpu
from jax.sharding import PartitionSpec as P

TILE = 256
ITERS_BEFORE = 2
ITERS_AFTER = 2
ITERS = ITERS_BEFORE + ITERS_AFTER

sigma_step = 0.35
tau_step = 0.35
fidelity = 1.0

SUB = 8
LANES = 128
TOP = 2 * SUB


def kernel(
    n_rows,
    n_cols,
    cost_ref,
    owner_ref,
    i_hbm,
    e_hbm,
    l_hbm,
    out_ref,
    img,
    edge,
    lab,
    u,
    v,
    p1,
    p2,
    wmap,
    colmask,
    rowmask,
    strip_out,
    strip_in,
    part_a,
    got_a,
    part_b,
    got_b,
    tiles,
    pack,
    recv,
    load_sem,
    strip_send,
    strip_recv,
    rim_send,
    rim_recv,
    a_send,
    a_recv,
    b_send,
    b_recv,
    t_send,
    t_recv,
):
    height, width = lab.shape
    wide = img.shape[1]
    tiles_down, tiles_across = height // TILE, width // TILE
    slots = out_ref.shape[0]
    r = lax.axis_index("rows")
    c = lax.axis_index("cols")
    own = pl.ds(TOP, height)
    chunks = height // SUB
    f32 = jnp.float32

    def local(src, dst, k):
        return pltpu.make_async_copy(src, dst, load_sem.at[k])

    loads = [
        local(l_hbm, lab, 0),
        local(i_hbm, img.at[own, pl.ds(0, width)], 1),
        local(e_hbm, edge.at[own, pl.ds(0, width)], 2),
    ]
    for load in loads:
        load.start()

    def row_peer(d):
        return (lax.rem(r + d, n_rows), c)

    def col_peer(d):
        return (r, lax.rem(c + d, n_cols))

    barrier = pltpu.get_barrier_semaphore()
    for d in range(1, n_rows):
        pl.semaphore_signal(barrier, inc=1, device_id=row_peer(d), device_id_type=pl.DeviceIdType.MESH)
    for d in range(1, n_cols):
        pl.semaphore_signal(barrier, inc=1, device_id=col_peer(d), device_id_type=pl.DeviceIdType.MESH)

    def remote(src, dst, send, got, peer):
        return pltpu.make_async_remote_copy(
            src_ref=src, dst_ref=dst, send_sem=send, recv_sem=got,
            device_id=peer, device_id_type=pl.DeviceIdType.MESH,
        )

    lane = lax.broadcasted_iota(jnp.int32, (SUB, LANES), 1)
    sublane = lax.broadcasted_iota(jnp.int32, (SUB, LANES), 0)
    total_bands = n_rows * tiles_down
    total_across = n_cols * tiles_across
    for band in range(tiles_down + 2):
        tr = jnp.clip(r * tiles_down + band - 1, 0, total_bands - 1)
        for t in range(tiles_across):
            w = cost_ref[tr, c * tiles_across + t].astype(f32)
            for h in range(TILE // LANES):
                wmap[band * SUB:(band + 1) * SUB, t * TILE + h * LANES:t * TILE + (h + 1) * LANES] = (
                    jnp.full((SUB, LANES), w * (tau_step * fidelity), f32)
                )
        right = cost_ref[tr, jnp.clip((c + 1) * tiles_across, 0, total_across - 1)].astype(f32)
        left = cost_ref[tr, jnp.clip(c * tiles_across - 1, 0, total_across - 1)].astype(f32)
        wmap[band * SUB:(band + 1) * SUB, width:] = (
            jnp.where(lane < LANES // 2, jnp.full((SUB, LANES), right, f32), jnp.full((SUB, LANES), left, f32))
            * (tau_step * fidelity)
        )
    one = jnp.ones((SUB, LANES), f32)
    last_col = (c == n_cols - 1).astype(f32)
    first_col = (c == 0).astype(f32)
    last_row = (r == n_rows - 1).astype(f32)
    first_row = (r == 0).astype(f32)
    edge_lane = (lane == LANES - 1).astype(f32)
    edge_sub = (sublane == SUB - 1).astype(f32)
    colmask[:, :LANES] = one - edge_lane * last_col
    colmask[:, LANES:] = one - edge_lane * first_col

    def fill_rows(k, _):
        rowmask[pl.ds(k * SUB, SUB), :] = one
        return 0

    lax.fori_loop(0, chunks + 4, fill_rows, 0)
    rowmask[SUB:2 * SUB, :] = one - edge_sub * first_row
    rowmask[TOP + height - SUB:TOP + height, :] = one - edge_sub * last_row
    zero_wide = jnp.zeros((SUB, wide), f32)
    p1[0:SUB, :] = zero_wide
    u[0:SUB, :] = zero_wide
    bottom = slice(TOP + height + SUB, TOP + height + 2 * SUB)
    u[bottom, :] = zero_wide
    v[bottom, :] = zero_wide

    pl.semaphore_wait(barrier, n_rows + n_cols - 2)
    for load in loads:
        load.wait()

    left_cols = slice(0, LANES)
    right_cols = slice(width - LANES, width)
    for side, cols in enumerate((left_cols, right_cols)):
        take = slice(0, SUB) if side == 0 else slice(LANES - SUB, LANES)
        strip_out[side, 0:SUB, :] = lab[:, cols].astype(f32).T[take]
        strip_out[side, SUB:2 * SUB, :] = img[TOP:TOP + height, cols].T[take]
        strip_out[side, 2 * SUB:, :] = edge[TOP:TOP + height, cols].T[take]
    strips = [
        remote(strip_out.at[0], strip_in.at[0], strip_send.at[0], strip_recv.at[0], col_peer(n_cols - 1)),
        remote(strip_out.at[1], strip_in.at[1], strip_send.at[1], strip_recv.at[1], col_peer(1)),
    ]
    for strip in strips:
        strip.start()

    zero = jnp.zeros((SUB, LANES), f32)

    def lane_sum(x):
        total = x[:, :LANES]
        for k in range(1, width // LANES):
            total = total + x[:, k * LANES:(k + 1) * LANES]
        return total

    def add_sums(acc, field, image):
        rest = 1.0 - field
        return (
            acc[0] + lane_sum(field * image),
            acc[1] + lane_sum(field),
            acc[2] + lane_sum(rest * image),
            acc[3] + lane_sum(rest),
        )

    def first(k, acc):
        rows = pl.ds(pl.multiple_of(TOP + k * SUB, SUB), SUB)
        field = lab[pl.ds(pl.multiple_of(k * SUB, SUB), SUB), :].astype(f32)
        u[rows, :width] = field
        return add_sums(acc, field, img[rows, :width])

    acc = lax.fori_loop(0, chunks, first, (zero,) * 4)

    def start_a(it, acc):
        stacked = jnp.concatenate([jnp.sum(x, axis=0, keepdims=True) for x in acc] + [zero[:SUB - 4]], axis=0)
        part_a[it] = stacked
        copies = [
            remote(part_a.at[it], got_a.at[it, d - 1], a_send.at[it, d - 1], a_recv.at[it, d - 1], row_peer(d))
            for d in range(1, n_rows)
        ]
        for copy in copies:
            copy.start()
        return copies

    def start_b(it, copies):
        for copy in copies:
            copy.wait()
        total = part_a[it]
        for d in range(n_rows - 1):
            total = total + got_a[it, d]
        part_b[it] = total
        copies = [
            remote(part_b.at[it], got_b.at[it, d - 1], b_send.at[it, d - 1], b_recv.at[it, d - 1], col_peer(d))
            for d in range(1, n_cols)
        ]
        for copy in copies:
            copy.start()
        return copies

    def means(it, copies):
        for copy in copies:
            copy.wait()
        total = part_b[it]
        for d in range(n_cols - 1):
            total = total + got_b[it, d]
        sums = jnp.sum(total, axis=1, keepdims=True)
        return (sums[0:1] / sums[1:2], sums[2:3] / sums[3:4])

    pending = start_a(0, acc)

    for strip in strips:
        strip.wait()
    middle = jnp.ones((LANES - 2 * SUB, height), f32)
    for k, buf in enumerate((u, img, edge)):
        part = slice(k * SUB, (k + 1) * SUB)
        buf[TOP:TOP + height, width:] = jnp.concatenate(
            [strip_in[0, part, :], middle, strip_in[1, part, :]], axis=0
        ).T
    rims = []
    for k, buf in enumerate((u, img, edge)):
        rims.append(remote(
            buf.at[pl.ds(TOP, SUB)], buf.at[pl.ds(TOP + height, SUB)],
            rim_send.at[2 * k], rim_recv.at[2 * k], row_peer(n_rows - 1)))
        rims.append(remote(
            buf.at[pl.ds(TOP + height - SUB, SUB)], buf.at[pl.ds(TOP - SUB, SUB)],
            rim_send.at[2 * k + 1], rim_recv.at[2 * k + 1], row_peer(1)))
    for rim in rims:
        rim.start()
    for rim in rims:
        rim.wait()

    def band_of(k):
        return (k - 2 + TILE // SUB) // (TILE // SUB)

    def weights(k):
        return wmap[pl.ds(pl.multiple_of(band_of(k) * SUB, SUB), SUB), :]

    wide_sub = lax.broadcasted_iota(jnp.int32, (SUB, wide), 0)

    def dual(it, k):
        base = pl.multiple_of(k * SUB, SUB)
        rows = pl.ds(base, SUB)
        source = u if it == 0 else v
        here = source[rows, :]
        below = source[pl.ds(pl.multiple_of(base + SUB, SUB), SUB), :]
        gx = pltpu.roll(jnp.where(wide_sub == 0, below, here), SUB - 1, 0) - here
        gy = pltpu.roll(here, wide - 1, 1) - here
        if it == 0:
            q1, q2 = gx * sigma_step, gy * sigma_step
        else:
            old1, old2 = p1[rows, :], p2[rows, :]
            q1, q2 = old1 + gx, old2 + gy
        q1 = q1 * jnp.concatenate([rowmask[rows, :]] * (wide // LANES), axis=1)
        cut = width - LANES
        q2 = jnp.concatenate([q2[:, :cut], q2[:, cut:] * colmask[...]], axis=1)
        shrink = jnp.minimum(1.0, edge[rows, :] * lax.rsqrt(q1 * q1 + q2 * q2))
        q1, q2 = q1 * shrink, q2 * shrink
        if it >= ITERS_BEFORE:
            live = weights(k) > 0.0
            q1, q2 = jnp.where(live, q1, old1), jnp.where(live, q2, old2)
        p1[rows, :] = q1
        p2[rows, :] = q2

    def primal(it, k, slope, middle_mean):
        base = pl.multiple_of(k * SUB, SUB)
        rows = pl.ds(base, SUB)
        old = u[rows, :]
        image = img[rows, :]
        here1, here2 = p1[rows, :], p2[rows, :]
        above = p1[pl.ds(pl.multiple_of(base - SUB, SUB), SUB), :]
        shifted = pltpu.roll(jnp.where(wide_sub == SUB - 1, above, here1), 1, 0)
        div = (here1 - shifted) + (here2 - pltpu.roll(here2, 1, 1))
        w = weights(k)
        new = jnp.clip(old + (div * tau_step - w * (slope * (image - middle_mean))), 0.0, 1.0)
        if it >= ITERS_BEFORE:
            new = jnp.where(w > 0.0, new, old)
        return old, new, image, w

    for it in range(ITERS):
        half = chunks // 2 + 2

        def dual_loop(lo, hi):
            def step(k, _):
                dual(it, k)
                return 0
            lax.fori_loop(lo, hi, step, 0)

        dual_loop(1, half)
        pending = start_b(it, pending)
        dual_loop(half, chunks + 3)
        c1, c2 = means(it, pending)
        slope = 2.0 * (c2 - c1)
        middle_mean = 0.5 * (c1 + c2)

        def update(k):
            old, new, image, w = primal(it, k, slope, middle_mean)
            rows = pl.ds(pl.multiple_of(k * SUB, SUB), SUB)
            ahead = new + (new - old)
            if it == ITERS_BEFORE - 1:
                ahead = jnp.where(w > 0.0, ahead, new)
            u[rows, :] = new
            v[rows, :] = ahead * sigma_step
            return new, image

        if it < ITERS - 1:
            update(1)

            def step(k, acc):
                new, image = update(k)
                return add_sums(acc, new[:, :width], image[:, :width])

            acc = lax.fori_loop(2, chunks + 2, step, (zero,) * 4)
            pending = start_a(it + 1, acc)
            update(chunks + 2)
        else:
            def last(k, _):
                new = primal(it, k, slope, middle_mean)[1]
                row = (k - 2) // (TILE // SUB)
                at = pl.ds(pl.multiple_of(lax.rem(k - 2, TILE // SUB) * SUB, SUB), SUB)
                for t in range(tiles_across):
                    tiles[row * tiles_across + t, at, :] = new[:, t * TILE:(t + 1) * TILE]
                return 0

            lax.fori_loop(2, chunks + 2, last, 0)

    own_owner = [
        owner_ref[r * tiles_down + a, c * tiles_across + b]
        for a in range(tiles_down) for b in range(tiles_across)
    ]
    step_rows = 32

    def fill(dst, k):
        source = jnp.int32(0)
        used = jnp.int32(0)
        for t, o in enumerate(own_owner):
            hit = (o >= k * slots) & (o < (k + 1) * slots)
            source = jnp.where(hit, t, source)
            used = jnp.where(hit, 1, used)
        scale = used.astype(f32)

        def step(j, _):
            at = pl.ds(pl.multiple_of(j * step_rows, step_rows), step_rows)
            dst[at, :] = tiles[source, at, :] * scale
            return 0

        lax.fori_loop(0, TILE // step_rows, step, 0)

    sends = []
    for d in list(range(1, n_rows)):
        fill(pack.at[d - 1], lax.rem(r + d, n_rows))
        copy = remote(pack.at[d - 1], recv.at[r], t_send.at[d - 1], t_recv.at[d - 1], row_peer(d))
        copy.start()
        sends.append(copy)
    fill(recv.at[r], r)

    origin = []
    for s in range(slots):
        def look(a, carry):
            source, used = carry
            for b in range(tiles_across):
                hit = owner_ref[a, c * tiles_across + b] == r * slots + s
                source = jnp.where(hit, a // tiles_down, source)
                used = jnp.where(hit, 1, used)
            return source, used
        origin.append(lax.fori_loop(0, total_bands, look, (jnp.int32(0), jnp.int32(0))))

    for copy in sends:
        copy.wait()
    for s in range(slots):
        source, used = origin[s]
        scale = used.astype(f32)

        def step(j, _):
            at = pl.ds(pl.multiple_of(j * step_rows, step_rows), step_rows)
            out_ref[s, 0, at, :] = recv[source, at, :] * scale
            return 0

        lax.fori_loop(0, TILE // step_rows, step, 0)


def body(n_rows, n_cols, intensity, edge_weight, labels, tile_cost, tile_owner):
    height, width = intensity.shape
    tiles_down, tiles_across = height // TILE, width // TILE
    slots = tiles_down * tiles_across // 2
    f32 = jnp.float32
    full = pltpu.VMEM((TOP + height + TOP, width + LANES), f32)
    dma = pltpu.SemaphoreType.DMA
    anywhere = pl.BlockSpec(memory_space=pl.ANY)
    smem = pl.BlockSpec(memory_space=pltpu.SMEM)
    return pl.pallas_call(
        functools.partial(kernel, n_rows, n_cols),
        out_shape=jax.ShapeDtypeStruct((slots, 1, TILE, TILE), f32),
        in_specs=[smem, smem, anywhere, anywhere, anywhere],
        out_specs=pl.BlockSpec(memory_space=pltpu.VMEM),
        scratch_shapes=[
            full,
            full,
            pltpu.VMEM((height, width), jnp.int32),
            full,
            full,
            full,
            full,
            pltpu.VMEM(((tiles_down + 2) * SUB, width + LANES), f32),
            pltpu.VMEM((SUB, 2 * LANES), f32),
            pltpu.VMEM((TOP + height + TOP, LANES), f32),
            pltpu.VMEM((2, 3 * SUB, height), f32),
            pltpu.VMEM((2, 3 * SUB, height), f32),
            pltpu.VMEM((ITERS, SUB, LANES), f32),
            pltpu.VMEM((ITERS, n_rows - 1, SUB, LANES), f32),
            pltpu.VMEM((ITERS, SUB, LANES), f32),
            pltpu.VMEM((ITERS, n_cols - 1, SUB, LANES), f32),
            pltpu.VMEM((tiles_down * tiles_across, TILE, TILE), f32),
            pltpu.VMEM((n_rows - 1, TILE, TILE), f32),
            pltpu.VMEM((n_rows, TILE, TILE), f32),
            dma((3,)),
            dma((2,)),
            dma((2,)),
            dma((6,)),
            dma((6,)),
            dma((ITERS, n_rows - 1)),
            dma((ITERS, n_rows - 1)),
            dma((ITERS, n_cols - 1)),
            dma((ITERS, n_cols - 1)),
            dma((n_rows - 1,)),
            dma((n_rows - 1,)),
        ],
        compiler_params=pltpu.CompilerParams(
            collective_id=0, has_side_effects=True, vmem_limit_bytes=56 * 1024 * 1024
        ),
    )(tile_cost, tile_owner, intensity, edge_weight, labels)


def solution(mesh):
    return jax.shard_map(
        functools.partial(body, mesh.shape["rows"], mesh.shape["cols"]),
        mesh=mesh,
        in_specs=(P("rows", "cols"), P("rows", "cols"), P("rows", "cols"), P(), P()),
        out_specs=P("rows", "cols", None, None),
        check_vma=False,
    )
```

```python
import functools

import jax
import jax.numpy as jnp
from jax import lax
from jax.experimental import pallas as pl
from jax.experimental.pallas import tpu as pltpu
from jax.sharding import PartitionSpec as P

TILE = 256
ITERS_BEFORE = 2
ITERS_AFTER = 2
ITERS = ITERS_BEFORE + ITERS_AFTER

sigma_step = 0.35
tau_step = 0.35
fidelity = 1.0

SUB = 8
LANES = 128
BATCH = 4
TOP = 2 * SUB


def kernel(
    n_rows,
    n_cols,
    cost_ref,
    owner_ref,
    i_hbm,
    e_hbm,
    l_hbm,
    out_ref,
    img,
    edge,
    lab,
    u,
    v,
    p1,
    p2,
    wmap,
    colmask,
    rowmask,
    strip_out,
    strip_in,
    part_a,
    got_a,
    part_b,
    got_b,
    tiles,
    pack,
    recv,
    load_sem,
    strip_send,
    strip_recv,
    rim_send,
    rim_recv,
    a_send,
    a_recv,
    b_send,
    b_recv,
    t_send,
    t_recv,
):
    height, width = lab.shape
    wide = img.shape[1]
    tiles_down, tiles_across = height // TILE, width // TILE
    slots = out_ref.shape[0]
    r = lax.axis_index("rows")
    c = lax.axis_index("cols")
    own = pl.ds(TOP, height)
    chunks = height // SUB
    f32 = jnp.float32

    def local(src, dst, k):
        return pltpu.make_async_copy(src, dst, load_sem.at[k])

    loads = [
        local(l_hbm, lab, 0),
        local(i_hbm, img.at[own, pl.ds(0, width)], 1),
        local(e_hbm, edge.at[own, pl.ds(0, width)], 2),
    ]
    for load in loads:
        load.start()

    def row_peer(d):
        return (lax.rem(r + d, n_rows), c)

    def col_peer(d):
        return (r, lax.rem(c + d, n_cols))

    barrier = pltpu.get_barrier_semaphore()
    for d in range(1, n_rows):
        pl.semaphore_signal(barrier, inc=1, device_id=row_peer(d), device_id_type=pl.DeviceIdType.MESH)
    for d in range(1, n_cols):
        pl.semaphore_signal(barrier, inc=1, device_id=col_peer(d), device_id_type=pl.DeviceIdType.MESH)

    def remote(src, dst, send, got, peer):
        return pltpu.make_async_remote_copy(
            src_ref=src, dst_ref=dst, send_sem=send, recv_sem=got,
            device_id=peer, device_id_type=pl.DeviceIdType.MESH,
        )

    lane = lax.broadcasted_iota(jnp.int32, (SUB, LANES), 1)
    sublane = lax.broadcasted_iota(jnp.int32, (SUB, LANES), 0)
    total_bands = n_rows * tiles_down
    total_across = n_cols * tiles_across
    for band in range(tiles_down + 2):
        tr = jnp.clip(r * tiles_down + band - 1, 0, total_bands - 1)
        for t in range(tiles_across):
            w = cost_ref[tr, c * tiles_across + t].astype(f32)
            for h in range(TILE // LANES):
                wmap[band * SUB:(band + 1) * SUB, t * TILE + h * LANES:t * TILE + (h + 1) * LANES] = (
                    jnp.full((SUB, LANES), w * (tau_step * fidelity), f32)
                )
        right = cost_ref[tr, jnp.clip((c + 1) * tiles_across, 0, total_across - 1)].astype(f32)
        left = cost_ref[tr, jnp.clip(c * tiles_across - 1, 0, total_across - 1)].astype(f32)
        wmap[band * SUB:(band + 1) * SUB, width:] = (
            jnp.where(lane < LANES // 2, jnp.full((SUB, LANES), right, f32), jnp.full((SUB, LANES), left, f32))
            * (tau_step * fidelity)
        )
    one = jnp.ones((SUB, LANES), f32)
    last_col = (c == n_cols - 1).astype(f32)
    first_col = (c == 0).astype(f32)
    last_row = (r == n_rows - 1).astype(f32)
    first_row = (r == 0).astype(f32)
    edge_lane = (lane == LANES - 1).astype(f32)
    edge_sub = (sublane == SUB - 1).astype(f32)
    colmask[:, :LANES] = one - edge_lane * last_col
    colmask[:, LANES:] = one - edge_lane * first_col

    def fill_rows(k, _):
        rowmask[pl.ds(k * SUB, SUB), :] = one
        return 0

    lax.fori_loop(0, chunks + 4, fill_rows, 0)
    rowmask[SUB:2 * SUB, :] = one - edge_sub * first_row
    rowmask[TOP + height - SUB:TOP + height, :] = one - edge_sub * last_row
    zero_wide = jnp.zeros((SUB, wide), f32)
    p1[0:SUB, :] = zero_wide
    u[0:SUB, :] = zero_wide
    bottom = slice(TOP + height + SUB, TOP + height + 2 * SUB)
    u[bottom, :] = zero_wide
    v[bottom, :] = zero_wide

    pl.semaphore_wait(barrier, n_rows + n_cols - 2)
    for load in loads:
        load.wait()

    left_cols = slice(0, LANES)
    right_cols = slice(width - LANES, width)
    for side, cols in enumerate((left_cols, right_cols)):
        take = slice(0, SUB) if side == 0 else slice(LANES - SUB, LANES)
        strip_out[side, 0:SUB, :] = lab[:, cols].astype(f32).T[take]
        strip_out[side, SUB:2 * SUB, :] = img[TOP:TOP + height, cols].T[take]
        strip_out[side, 2 * SUB:, :] = edge[TOP:TOP + height, cols].T[take]
    strips = [
        remote(strip_out.at[0], strip_in.at[0], strip_send.at[0], strip_recv.at[0], col_peer(n_cols - 1)),
        remote(strip_out.at[1], strip_in.at[1], strip_send.at[1], strip_recv.at[1], col_peer(1)),
    ]
    for strip in strips:
        strip.start()

    zero = jnp.zeros((SUB, LANES), f32)

    def lane_sum(x):
        total = x[:, :LANES]
        for k in range(1, width // LANES):
            total = total + x[:, k * LANES:(k + 1) * LANES]
        return total

    def add_sums(acc, field, image):
        rest = 1.0 - field
        return (
            acc[0] + lane_sum(field * image),
            acc[1] + lane_sum(field),
            acc[2] + lane_sum(rest * image),
            acc[3] + lane_sum(rest),
        )

    def first(k, acc):
        rows = pl.ds(pl.multiple_of(TOP + k * SUB, SUB), SUB)
        field = lab[pl.ds(pl.multiple_of(k * SUB, SUB), SUB), :].astype(f32)
        u[rows, :width] = field
        return add_sums(acc, field, img[rows, :width])

    acc = lax.fori_loop(0, chunks, first, (zero,) * 4, unroll=4)

    def start_a(it, acc):
        stacked = jnp.concatenate([jnp.sum(x, axis=0, keepdims=True) for x in acc] + [zero[:SUB - 4]], axis=0)
        part_a[it] = stacked
        copies = [
            remote(part_a.at[it], got_a.at[it, d - 1], a_send.at[it, d - 1], a_recv.at[it, d - 1], row_peer(d))
            for d in range(1, n_rows)
        ]
        for copy in copies:
            copy.start()
        return copies

    def start_b(it, copies):
        for copy in copies:
            copy.wait()
        total = part_a[it]
        for d in range(n_rows - 1):
            total = total + got_a[it, d]
        part_b[it] = total
        copies = [
            remote(part_b.at[it], got_b.at[it, d - 1], b_send.at[it, d - 1], b_recv.at[it, d - 1], col_peer(d))
            for d in range(1, n_cols)
        ]
        for copy in copies:
            copy.start()
        return copies

    def means(it, copies):
        for copy in copies:
            copy.wait()
        total = part_b[it]
        for d in range(n_cols - 1):
            total = total + got_b[it, d]
        sums = jnp.sum(total, axis=1, keepdims=True)
        return (sums[0:1] / sums[1:2], sums[2:3] / sums[3:4])

    pending = start_a(0, acc)

    for strip in strips:
        strip.wait()
    middle = jnp.ones((LANES - 2 * SUB, height), f32)
    for k, buf in enumerate((u, img, edge)):
        part = slice(k * SUB, (k + 1) * SUB)
        buf[TOP:TOP + height, width:] = jnp.concatenate(
            [strip_in[0, part, :], middle, strip_in[1, part, :]], axis=0
        ).T
    rims = []
    for k, buf in enumerate((u, img, edge)):
        rims.append(remote(
            buf.at[pl.ds(TOP, SUB)], buf.at[pl.ds(TOP + height, SUB)],
            rim_send.at[2 * k], rim_recv.at[2 * k], row_peer(n_rows - 1)))
        rims.append(remote(
            buf.at[pl.ds(TOP + height - SUB, SUB)], buf.at[pl.ds(TOP - SUB, SUB)],
            rim_send.at[2 * k + 1], rim_recv.at[2 * k + 1], row_peer(1)))
    for rim in rims:
        rim.start()
    for rim in rims:
        rim.wait()

    def band_of(k):
        return (k - 2 + TILE // SUB) // (TILE // SUB)

    def weights(k):
        return wmap[pl.ds(pl.multiple_of(band_of(k) * SUB, SUB), SUB), :]

    wide_sub = lax.broadcasted_iota(jnp.int32, (SUB, wide), 0)

    def rows_at(start, j):
        base = pl.multiple_of(start * SUB, SUB)
        return pl.ds(pl.multiple_of(base + j * SUB, SUB), SUB)

    def dual(it, start, count):
        source = u if it == 0 else v
        fields = [source[rows_at(start, j), :] for j in range(count + 1)]
        cut = width - LANES
        results = []
        for j in range(count):
            rows = rows_at(start, j)
            here = fields[j]
            gx = pltpu.roll(jnp.where(wide_sub == 0, fields[j + 1], here), SUB - 1, 0) - here
            gy = pltpu.roll(here, wide - 1, 1) - here
            if it == 0:
                q1, q2 = gx * sigma_step, gy * sigma_step
            else:
                old1, old2 = p1[rows, :], p2[rows, :]
                q1, q2 = old1 + gx, old2 + gy
            q1 = q1 * jnp.concatenate([rowmask[rows, :]] * (wide // LANES), axis=1)
            q2 = jnp.concatenate([q2[:, :cut], q2[:, cut:] * colmask[...]], axis=1)
            shrink = jnp.minimum(1.0, edge[rows, :] * lax.rsqrt(q1 * q1 + q2 * q2))
            q1, q2 = q1 * shrink, q2 * shrink
            if it >= ITERS_BEFORE:
                live = weights(start + j) > 0.0
                q1, q2 = jnp.where(live, q1, old1), jnp.where(live, q2, old2)
            results.append((q1, q2))
        for j, (q1, q2) in enumerate(results):
            p1[rows_at(start, j), :] = q1
            p2[rows_at(start, j), :] = q2

    def primal(it, start, count, slope, middle_mean):
        duals = [p1[rows_at(start, j), :] for j in range(-1, count)]
        results = []
        for j in range(count):
            rows = rows_at(start, j)
            old = u[rows, :]
            image = img[rows, :]
            here1, here2 = duals[j + 1], p2[rows, :]
            shifted = pltpu.roll(jnp.where(wide_sub == SUB - 1, duals[j], here1), 1, 0)
            div = (here1 - shifted) + (here2 - pltpu.roll(here2, 1, 1))
            w = weights(start + j)
            new = jnp.clip(old + (div * tau_step - w * (slope * (image - middle_mean))), 0.0, 1.0)
            if it >= ITERS_BEFORE:
                new = jnp.where(w > 0.0, new, old)
            results.append((old, new, image, w))
        return results

    for it in range(ITERS):
        half = chunks // 2 + 2

        def dual_loop(lo, hi):
            whole = (hi - lo) // BATCH

            def step(k, _):
                dual(it, lo + k * BATCH, BATCH)
                return 0
            lax.fori_loop(0, whole, step, 0)
            if lo + whole * BATCH < hi:
                dual(it, lo + whole * BATCH, hi - lo - whole * BATCH)

        dual_loop(1, half)
        pending = start_b(it, pending)
        dual_loop(half, chunks + 3)
        c1, c2 = means(it, pending)
        slope = 2.0 * (c2 - c1)
        middle_mean = 0.5 * (c1 + c2)

        def update(start, count):
            results = primal(it, start, count, slope, middle_mean)
            for j, (old, new, image, w) in enumerate(results):
                ahead = new + (new - old)
                if it == ITERS_BEFORE - 1:
                    ahead = jnp.where(w > 0.0, ahead, new)
                u[rows_at(start, j), :] = new
                v[rows_at(start, j), :] = ahead * sigma_step
            return results

        if it < ITERS - 1:
            update(1, 1)

            def step(k, acc):
                for _, new, image, _ in update(2 + k * BATCH, BATCH):
                    acc = add_sums(acc, new[:, :width], image[:, :width])
                return acc

            acc = lax.fori_loop(0, chunks // BATCH, step, (zero,) * 4)
            pending = start_a(it + 1, acc)
            update(chunks + 2, 1)
        else:
            def last(k, _):
                results = primal(it, 2 + k * BATCH, BATCH, slope, middle_mean)
                per_tile = TILE // SUB // BATCH
                row = k // per_tile
                for j, (_, new, _, _) in enumerate(results):
                    at = pl.ds(pl.multiple_of(lax.rem(k, per_tile) * (BATCH * SUB) + j * SUB, SUB), SUB)
                    for t in range(tiles_across):
                        tiles[row * tiles_across + t, at, :] = new[:, t * TILE:(t + 1) * TILE]
                return 0

            lax.fori_loop(0, chunks // BATCH, last, 0)

    own_owner = [
        owner_ref[r * tiles_down + a, c * tiles_across + b]
        for a in range(tiles_down) for b in range(tiles_across)
    ]
    step_rows = 32

    def fill(dst, k):
        source = jnp.int32(0)
        used = jnp.int32(0)
        for t, o in enumerate(own_owner):
            hit = (o >= k * slots) & (o < (k + 1) * slots)
            source = jnp.where(hit, t, source)
            used = jnp.where(hit, 1, used)
        scale = used.astype(f32)

        def step(j, _):
            at = pl.ds(pl.multiple_of(j * step_rows, step_rows), step_rows)
            dst[at, :] = tiles[source, at, :] * scale
            return 0

        lax.fori_loop(0, TILE // step_rows, step, 0)

    sends = []
    for d in list(range(1, n_rows)):
        fill(pack.at[d - 1], lax.rem(r + d, n_rows))
        copy = remote(pack.at[d - 1], recv.at[r], t_send.at[d - 1], t_recv.at[d - 1], row_peer(d))
        copy.start()
        sends.append(copy)
    fill(recv.at[r], r)

    origin = []
    for s in range(slots):
        def look(a, carry):
            source, used = carry
            for b in range(tiles_across):
                hit = owner_ref[a, c * tiles_across + b] == r * slots + s
                source = jnp.where(hit, a // tiles_down, source)
                used = jnp.where(hit, 1, used)
            return source, used
        origin.append(lax.fori_loop(0, total_bands, look, (jnp.int32(0), jnp.int32(0))))

    for copy in sends:
        copy.wait()
    for s in range(slots):
        source, used = origin[s]
        scale = used.astype(f32)

        def step(j, _):
            at = pl.ds(pl.multiple_of(j * step_rows, step_rows), step_rows)
            out_ref[s, 0, at, :] = recv[source, at, :] * scale
            return 0

        lax.fori_loop(0, TILE // step_rows, step, 0)


def body(n_rows, n_cols, intensity, edge_weight, labels, tile_cost, tile_owner):
    height, width = intensity.shape
    tiles_down, tiles_across = height // TILE, width // TILE
    slots = tiles_down * tiles_across // 2
    f32 = jnp.float32
    full = pltpu.VMEM((TOP + height + TOP, width + LANES), f32)
    dma = pltpu.SemaphoreType.DMA
    anywhere = pl.BlockSpec(memory_space=pl.ANY)
    smem = pl.BlockSpec(memory_space=pltpu.SMEM)
    return pl.pallas_call(
        functools.partial(kernel, n_rows, n_cols),
        out_shape=jax.ShapeDtypeStruct((slots, 1, TILE, TILE), f32),
        in_specs=[smem, smem, anywhere, anywhere, anywhere],
        out_specs=pl.BlockSpec(memory_space=pltpu.VMEM),
        scratch_shapes=[
            full,
            full,
            pltpu.VMEM((height, width), jnp.int32),
            full,
            full,
            full,
            full,
            pltpu.VMEM(((tiles_down + 2) * SUB, width + LANES), f32),
            pltpu.VMEM((SUB, 2 * LANES), f32),
            pltpu.VMEM((TOP + height + TOP, LANES), f32),
            pltpu.VMEM((2, 3 * SUB, height), f32),
            pltpu.VMEM((2, 3 * SUB, height), f32),
            pltpu.VMEM((ITERS, SUB, LANES), f32),
            pltpu.VMEM((ITERS, n_rows - 1, SUB, LANES), f32),
            pltpu.VMEM((ITERS, SUB, LANES), f32),
            pltpu.VMEM((ITERS, n_cols - 1, SUB, LANES), f32),
            pltpu.VMEM((tiles_down * tiles_across, TILE, TILE), f32),
            pltpu.VMEM((n_rows - 1, TILE, TILE), f32),
            pltpu.VMEM((n_rows, TILE, TILE), f32),
            dma((3,)),
            dma((2,)),
            dma((2,)),
            dma((6,)),
            dma((6,)),
            dma((ITERS, n_rows - 1)),
            dma((ITERS, n_rows - 1)),
            dma((ITERS, n_cols - 1)),
            dma((ITERS, n_cols - 1)),
            dma((n_rows - 1,)),
            dma((n_rows - 1,)),
        ],
        compiler_params=pltpu.CompilerParams(
            collective_id=0, has_side_effects=True, vmem_limit_bytes=56 * 1024 * 1024
        ),
    )(tile_cost, tile_owner, intensity, edge_weight, labels)


def solution(mesh):
    return jax.shard_map(
        functools.partial(body, mesh.shape["rows"], mesh.shape["cols"]),
        mesh=mesh,
        in_specs=(P("rows", "cols"), P("rows", "cols"), P("rows", "cols"), P(), P()),
        out_specs=P("rows", "cols", None, None),
        check_vma=False,
    )
```

```python
import functools

import jax
import jax.numpy as jnp
from jax import lax
from jax.experimental import pallas as pl
from jax.experimental.pallas import tpu as pltpu
from jax.sharding import PartitionSpec as P

TILE = 256
ITERS_BEFORE = 2
ITERS_AFTER = 2
ITERS = ITERS_BEFORE + ITERS_AFTER

sigma_step = 0.35
tau_step = 0.35
fidelity = 1.0

SUB = 8
LANES = 128
BATCH = 4
TOP = 2 * SUB


def kernel(
    n_rows,
    n_cols,
    cost_ref,
    owner_ref,
    i_hbm,
    e_hbm,
    l_hbm,
    out_ref,
    img,
    edge,
    lab,
    u,
    v,
    p1,
    p2,
    moved,
    wmap,
    colmask,
    rowmask,
    strip_out,
    strip_in,
    part_a,
    got_a,
    part_b,
    got_b,
    tiles,
    pack,
    recv,
    load_sem,
    strip_send,
    strip_recv,
    rim_send,
    rim_recv,
    a_send,
    a_recv,
    b_send,
    b_recv,
    t_send,
    t_recv,
):
    height, width = lab.shape
    wide = img.shape[1]
    tiles_down, tiles_across = height // TILE, width // TILE
    slots = out_ref.shape[0]
    r = lax.axis_index("rows")
    c = lax.axis_index("cols")
    own = pl.ds(TOP, height)
    chunks = height // SUB
    f32 = jnp.float32

    def local(src, dst, k):
        return pltpu.make_async_copy(src, dst, load_sem.at[k])

    loads = [
        local(l_hbm, lab, 0),
        local(i_hbm, img.at[own, pl.ds(0, width)], 1),
        local(e_hbm, edge.at[own, pl.ds(0, width)], 2),
    ]
    for load in loads:
        load.start()

    def row_peer(d):
        return (lax.rem(r + d, n_rows), c)

    def col_peer(d):
        return (r, lax.rem(c + d, n_cols))

    barrier = pltpu.get_barrier_semaphore()
    for d in range(1, n_rows):
        pl.semaphore_signal(barrier, inc=1, device_id=row_peer(d), device_id_type=pl.DeviceIdType.MESH)
    for d in range(1, n_cols):
        pl.semaphore_signal(barrier, inc=1, device_id=col_peer(d), device_id_type=pl.DeviceIdType.MESH)

    def remote(src, dst, send, got, peer):
        return pltpu.make_async_remote_copy(
            src_ref=src, dst_ref=dst, send_sem=send, recv_sem=got,
            device_id=peer, device_id_type=pl.DeviceIdType.MESH,
        )

    lane = lax.broadcasted_iota(jnp.int32, (SUB, LANES), 1)
    sublane = lax.broadcasted_iota(jnp.int32, (SUB, LANES), 0)
    total_bands = n_rows * tiles_down
    total_across = n_cols * tiles_across
    for band in range(tiles_down + 2):
        tr = jnp.clip(r * tiles_down + band - 1, 0, total_bands - 1)
        for t in range(tiles_across):
            w = cost_ref[tr, c * tiles_across + t].astype(f32)
            for h in range(TILE // LANES):
                wmap[band * SUB:(band + 1) * SUB, t * TILE + h * LANES:t * TILE + (h + 1) * LANES] = (
                    jnp.full((SUB, LANES), w * (tau_step * fidelity), f32)
                )
        right = cost_ref[tr, jnp.clip((c + 1) * tiles_across, 0, total_across - 1)].astype(f32)
        left = cost_ref[tr, jnp.clip(c * tiles_across - 1, 0, total_across - 1)].astype(f32)
        wmap[band * SUB:(band + 1) * SUB, width:] = (
            jnp.where(lane < LANES // 2, jnp.full((SUB, LANES), right, f32), jnp.full((SUB, LANES), left, f32))
            * (tau_step * fidelity)
        )
    one = jnp.ones((SUB, LANES), f32)
    last_col = (c == n_cols - 1).astype(f32)
    first_col = (c == 0).astype(f32)
    last_row = (r == n_rows - 1).astype(f32)
    first_row = (r == 0).astype(f32)
    edge_lane = (lane == LANES - 1).astype(f32)
    edge_sub = (sublane == SUB - 1).astype(f32)
    colmask[:, :LANES] = one - edge_lane * last_col
    colmask[:, LANES:] = one - edge_lane * first_col

    def fill_rows(k, _):
        rowmask[pl.ds(k * SUB, SUB), :] = one
        return 0

    lax.fori_loop(0, chunks + 4, fill_rows, 0)
    rowmask[SUB:2 * SUB, :] = one - edge_sub * first_row
    rowmask[TOP + height - SUB:TOP + height, :] = one - edge_sub * last_row
    zero_wide = jnp.zeros((SUB, wide), f32)
    p1[0:SUB, :] = zero_wide
    u[0:SUB, :] = zero_wide
    bottom = slice(TOP + height + SUB, TOP + height + 2 * SUB)
    u[bottom, :] = zero_wide
    v[bottom, :] = zero_wide

    pl.semaphore_wait(barrier, n_rows + n_cols - 2)
    for load in loads:
        load.wait()

    left_cols = slice(0, LANES)
    right_cols = slice(width - LANES, width)
    for side, cols in enumerate((left_cols, right_cols)):
        take = slice(0, SUB) if side == 0 else slice(LANES - SUB, LANES)
        strip_out[side, 0:SUB, :] = lab[:, cols].astype(f32).T[take]
        strip_out[side, SUB:2 * SUB, :] = img[TOP:TOP + height, cols].T[take]
        strip_out[side, 2 * SUB:, :] = edge[TOP:TOP + height, cols].T[take]
    strips = [
        remote(strip_out.at[0], strip_in.at[0], strip_send.at[0], strip_recv.at[0], col_peer(n_cols - 1)),
        remote(strip_out.at[1], strip_in.at[1], strip_send.at[1], strip_recv.at[1], col_peer(1)),
    ]
    for strip in strips:
        strip.start()

    zero = jnp.zeros((SUB, LANES), f32)

    def lane_sum(x):
        total = x[:, :LANES]
        for k in range(1, width // LANES):
            total = total + x[:, k * LANES:(k + 1) * LANES]
        return total

    def add_sums(acc, field, image):
        rest = 1.0 - field
        return (
            acc[0] + lane_sum(field * image),
            acc[1] + lane_sum(field),
            acc[2] + lane_sum(rest * image),
            acc[3] + lane_sum(rest),
        )

    def first(k, acc):
        rows = pl.ds(pl.multiple_of(TOP + k * SUB, SUB), SUB)
        field = lab[pl.ds(pl.multiple_of(k * SUB, SUB), SUB), :].astype(f32)
        u[rows, :width] = field
        return add_sums(acc, field, img[rows, :width])

    acc = lax.fori_loop(0, chunks, first, (zero,) * 4, unroll=4)

    def start_a(it, acc):
        stacked = jnp.concatenate([jnp.sum(x, axis=0, keepdims=True) for x in acc] + [zero[:SUB - 4]], axis=0)
        part_a[it] = stacked
        copies = [
            remote(part_a.at[it], got_a.at[it, d - 1], a_send.at[it, d - 1], a_recv.at[it, d - 1], row_peer(d))
            for d in range(1, n_rows)
        ]
        for copy in copies:
            copy.start()
        return copies

    def start_b(it, copies):
        for copy in copies:
            copy.wait()
        total = part_a[it]
        for d in range(n_rows - 1):
            total = total + got_a[it, d]
        part_b[it] = total
        copies = [
            remote(part_b.at[it], got_b.at[it, d - 1], b_send.at[it, d - 1], b_recv.at[it, d - 1], col_peer(d))
            for d in range(1, n_cols)
        ]
        for copy in copies:
            copy.start()
        return copies

    def means(it, copies):
        for copy in copies:
            copy.wait()
        total = part_b[it]
        for d in range(n_cols - 1):
            total = total + got_b[it, d]
        sums = jnp.sum(total, axis=1, keepdims=True)
        return (sums[0:1] / sums[1:2], sums[2:3] / sums[3:4])

    pending = start_a(0, acc)

    for strip in strips:
        strip.wait()
    middle = jnp.ones((LANES - 2 * SUB, height), f32)
    for k, buf in enumerate((u, img, edge)):
        part = slice(k * SUB, (k + 1) * SUB)
        buf[TOP:TOP + height, width:] = jnp.concatenate(
            [strip_in[0, part, :], middle, strip_in[1, part, :]], axis=0
        ).T
    rims = []
    for k, buf in enumerate((u, img, edge)):
        rims.append(remote(
            buf.at[pl.ds(TOP, SUB)], buf.at[pl.ds(TOP + height, SUB)],
            rim_send.at[2 * k], rim_recv.at[2 * k], row_peer(n_rows - 1)))
        rims.append(remote(
            buf.at[pl.ds(TOP + height - SUB, SUB)], buf.at[pl.ds(TOP - SUB, SUB)],
            rim_send.at[2 * k + 1], rim_recv.at[2 * k + 1], row_peer(1)))
    for rim in rims:
        rim.start()
    for rim in rims:
        rim.wait()

    def band_of(k):
        return (k - 2 + TILE // SUB) // (TILE // SUB)

    def weights(k):
        return wmap[pl.ds(pl.multiple_of(band_of(k) * SUB, SUB), SUB), :]

    wide_sub = lax.broadcasted_iota(jnp.int32, (SUB, wide), 0)

    def rows_at(start, j):
        base = pl.multiple_of(start * SUB, SUB)
        return pl.ds(pl.multiple_of(base + j * SUB, SUB), SUB)

    def dual(it, start, count):
        source = u if it == 0 else v
        fields = [source[rows_at(start, j), :] for j in range(count + 1)]
        cut = width - LANES
        results = []
        for j in range(count):
            rows = rows_at(start, j)
            here = fields[j]
            gx = pltpu.roll(jnp.where(wide_sub == 0, fields[j + 1], here), SUB - 1, 0) - here
            gy = pltpu.roll(here, wide - 1, 1) - here
            if it == 0:
                q1, q2 = gx * sigma_step, gy * sigma_step
            else:
                old1, old2 = p1[rows, :], p2[rows, :]
                q1, q2 = old1 + gx, old2 + gy
            q1 = q1 * jnp.concatenate([rowmask[rows, :]] * (wide // LANES), axis=1)
            q2 = jnp.concatenate([q2[:, :cut], q2[:, cut:] * colmask[...]], axis=1)
            shrink = jnp.minimum(1.0, edge[rows, :] * lax.rsqrt(q1 * q1 + q2 * q2))
            q1, q2 = q1 * shrink, q2 * shrink
            if it >= ITERS_BEFORE:
                live = weights(start + j) > 0.0
                q1, q2 = jnp.where(live, q1, old1), jnp.where(live, q2, old2)
            results.append((q1, q2))
        before = p1[rows_at(start, -1), :]
        ahead = []
        for j, (q1, q2) in enumerate(results):
            shifted = pltpu.roll(jnp.where(wide_sub == SUB - 1, before, q1), 1, 0)
            div = (q1 - shifted) + (q2 - pltpu.roll(q2, 1, 1))
            old = fields[j] if it == 0 else u[rows_at(start, j), :]
            ahead.append(old + div * tau_step)
            before = q1
        for j, (q1, q2) in enumerate(results):
            rows = rows_at(start, j)
            p1[rows, :] = q1
            if it < ITERS - 1:
                p2[rows, :] = q2
            moved[rows, :] = ahead[j]

    def primal(it, start, count, slope, middle_mean):
        results = []
        for j in range(count):
            rows = rows_at(start, j)
            old = u[rows, :]
            image = img[rows, :]
            w = weights(start + j)
            new = jnp.clip(moved[rows, :] - w * (slope * (image - middle_mean)), 0.0, 1.0)
            if it >= ITERS_BEFORE:
                new = jnp.where(w > 0.0, new, old)
            results.append((old, new, image, w))
        return results

    for it in range(ITERS):
        half = chunks // 2 + 2

        def dual_loop(lo, hi):
            whole = (hi - lo) // BATCH

            def step(k, _):
                dual(it, lo + k * BATCH, BATCH)
                return 0
            lax.fori_loop(0, whole, step, 0)
            if lo + whole * BATCH < hi:
                dual(it, lo + whole * BATCH, hi - lo - whole * BATCH)

        dual_loop(1, half)
        pending = start_b(it, pending)
        dual_loop(half, chunks + 3)
        c1, c2 = means(it, pending)
        slope = 2.0 * (c2 - c1)
        middle_mean = 0.5 * (c1 + c2)

        def update(start, count):
            results = primal(it, start, count, slope, middle_mean)
            for j, (old, new, image, w) in enumerate(results):
                ahead = new + (new - old)
                if it == ITERS_BEFORE - 1:
                    ahead = jnp.where(w > 0.0, ahead, new)
                u[rows_at(start, j), :] = new
                v[rows_at(start, j), :] = ahead * sigma_step
            return results

        if it < ITERS - 1:
            update(1, 1)

            def step(k, acc):
                for _, new, image, _ in update(2 + k * BATCH, BATCH):
                    acc = add_sums(acc, new[:, :width], image[:, :width])
                return acc

            acc = lax.fori_loop(0, chunks // BATCH, step, (zero,) * 4)
            pending = start_a(it + 1, acc)
            update(chunks + 2, 1)
        else:
            def last(k, _):
                results = primal(it, 2 + k * BATCH, BATCH, slope, middle_mean)
                per_tile = TILE // SUB // BATCH
                row = k // per_tile
                for j, (_, new, _, _) in enumerate(results):
                    at = pl.ds(pl.multiple_of(lax.rem(k, per_tile) * (BATCH * SUB) + j * SUB, SUB), SUB)
                    for t in range(tiles_across):
                        tiles[row * tiles_across + t, at, :] = new[:, t * TILE:(t + 1) * TILE]
                return 0

            lax.fori_loop(0, chunks // BATCH, last, 0)

    own_owner = [
        owner_ref[r * tiles_down + a, c * tiles_across + b]
        for a in range(tiles_down) for b in range(tiles_across)
    ]
    step_rows = 32

    def fill(dst, k):
        source = jnp.int32(0)
        used = jnp.int32(0)
        for t, o in enumerate(own_owner):
            hit = (o >= k * slots) & (o < (k + 1) * slots)
            source = jnp.where(hit, t, source)
            used = jnp.where(hit, 1, used)
        scale = used.astype(f32)

        def step(j, _):
            at = pl.ds(pl.multiple_of(j * step_rows, step_rows), step_rows)
            dst[at, :] = tiles[source, at, :] * scale
            return 0

        lax.fori_loop(0, TILE // step_rows, step, 0)

    sends = []
    for d in list(range(1, n_rows)):
        fill(pack.at[d - 1], lax.rem(r + d, n_rows))
        copy = remote(pack.at[d - 1], recv.at[r], t_send.at[d - 1], t_recv.at[d - 1], row_peer(d))
        copy.start()
        sends.append(copy)
    fill(recv.at[r], r)

    origin = []
    for s in range(slots):
        def look(a, carry):
            source, used = carry
            for b in range(tiles_across):
                hit = owner_ref[a, c * tiles_across + b] == r * slots + s
                source = jnp.where(hit, a // tiles_down, source)
                used = jnp.where(hit, 1, used)
            return source, used
        origin.append(lax.fori_loop(0, total_bands, look, (jnp.int32(0), jnp.int32(0))))

    for copy in sends:
        copy.wait()
    for s in range(slots):
        source, used = origin[s]
        scale = used.astype(f32)

        def step(j, _):
            at = pl.ds(pl.multiple_of(j * step_rows, step_rows), step_rows)
            out_ref[s, 0, at, :] = recv[source, at, :] * scale
            return 0

        lax.fori_loop(0, TILE // step_rows, step, 0)


def body(n_rows, n_cols, intensity, edge_weight, labels, tile_cost, tile_owner):
    height, width = intensity.shape
    tiles_down, tiles_across = height // TILE, width // TILE
    slots = tiles_down * tiles_across // 2
    f32 = jnp.float32
    full = pltpu.VMEM((TOP + height + TOP, width + LANES), f32)
    dma = pltpu.SemaphoreType.DMA
    anywhere = pl.BlockSpec(memory_space=pl.ANY)
    smem = pl.BlockSpec(memory_space=pltpu.SMEM)
    return pl.pallas_call(
        functools.partial(kernel, n_rows, n_cols),
        out_shape=jax.ShapeDtypeStruct((slots, 1, TILE, TILE), f32),
        in_specs=[smem, smem, anywhere, anywhere, anywhere],
        out_specs=pl.BlockSpec(memory_space=pltpu.VMEM),
        scratch_shapes=[
            full,
            full,
            pltpu.VMEM((height, width), jnp.int32),
            full,
            full,
            full,
            full,
            full,
            pltpu.VMEM(((tiles_down + 2) * SUB, width + LANES), f32),
            pltpu.VMEM((SUB, 2 * LANES), f32),
            pltpu.VMEM((TOP + height + TOP, LANES), f32),
            pltpu.VMEM((2, 3 * SUB, height), f32),
            pltpu.VMEM((2, 3 * SUB, height), f32),
            pltpu.VMEM((ITERS, SUB, LANES), f32),
            pltpu.VMEM((ITERS, n_rows - 1, SUB, LANES), f32),
            pltpu.VMEM((ITERS, SUB, LANES), f32),
            pltpu.VMEM((ITERS, n_cols - 1, SUB, LANES), f32),
            pltpu.VMEM((tiles_down * tiles_across, TILE, TILE), f32),
            pltpu.VMEM((n_rows - 1, TILE, TILE), f32),
            pltpu.VMEM((n_rows, TILE, TILE), f32),
            dma((3,)),
            dma((2,)),
            dma((2,)),
            dma((6,)),
            dma((6,)),
            dma((ITERS, n_rows - 1)),
            dma((ITERS, n_rows - 1)),
            dma((ITERS, n_cols - 1)),
            dma((ITERS, n_cols - 1)),
            dma((n_rows - 1,)),
            dma((n_rows - 1,)),
        ],
        compiler_params=pltpu.CompilerParams(
            collective_id=0, has_side_effects=True, vmem_limit_bytes=56 * 1024 * 1024
        ),
    )(tile_cost, tile_owner, intensity, edge_weight, labels)


def solution(mesh):
    return jax.shard_map(
        functools.partial(body, mesh.shape["rows"], mesh.shape["cols"]),
        mesh=mesh,
        in_specs=(P("rows", "cols"), P("rows", "cols"), P("rows", "cols"), P(), P()),
        out_specs=P("rows", "cols", None, None),
        check_vma=False,
    )
```
